32 devices in a mesh: seq: 8 (over y, x, core), kvh: 4 (over z).
Axes of the slice: x: 2, y: 2, z: 4, core: 2. Of those that a mesh axis runs over, the one named last changes fastest.
Arguments:
- hidden: bfloat16 [6144, 4096], P('seq'), may hold values from -32 to 32
- w_query: bfloat16 [4096, 4096], P(None, 'kvh'), may hold values from -0.09375 to 0.09375
- w_key: bfloat16 [4096, 1024], P(None, 'kvh'), may hold values from -0.09375 to 0.09375
- w_value: bfloat16 [4096, 1024], P(None, 'kvh'), may hold values from -0.09375 to 0.09375
- cached_key: bfloat16 [6144, 1024], P('seq', 'kvh'), may hold values from -6 to 6
- cached_value: bfloat16 [6144, 1024], P('seq', 'kvh'), may hold values from -6 to 6
- doc_lengths: int32 [4], replicated, may hold values from 1 to 3072, 6144 in all
- selected: int32 [960], replicated, may hold values from 0 to 767, as said below
Outputs:
- attended: bfloat16 [960, 4096], P('seq', 'kvh')
- score: float32 [6144], P('seq')
The draws below stay inside these ranges and needn't reach their ends.
Inputs may be any that keep to these rules, and one draw needn't show every extreme that they name: `selected`: each block of 120 entries holds distinct local row numbers in increasing order.
All inputs are finite; a program needn't handle non-finite values.
Results may differ from the reference program's by a relative error of at most 0.02.
Values may be sent and summed in bfloat16 or wider, within the bound.
A program may use at most 192 MiB of HBM per device.

```python
import math
import jax
import jax.numpy as jnp
import numpy as np
from jax import lax

D = 4096
HEADS = 32
KV_HEADS = 8
HEAD_DIM = 128
TOK_DEV = 768
DOCS = 4
SEL_DEV = 120
TOKENS = 6144
SELECTED = 960
DOC_MOST = 3072


def draw_selected(key, part):
    blocks = TOKENS // TOK_DEV
    block_keys = jax.random.split(key, blocks)

    def one_block(block_key):
        shuffled = jax.random.permutation(block_key, TOK_DEV)
        return jnp.sort(shuffled[:SEL_DEV]).astype(jnp.int32)
    return jax.vmap(one_block)(block_keys).reshape(-1).astype(jnp.int32)


def draw_hidden(key, part):
    base = jnp.clip(jax.random.normal(key, (TOKENS, D), jnp.float32), -4.0, 4.0)
    region_scale = jnp.exp(jax.random.uniform(jax.random.fold_in(key, 11), (16,), jnp.float32, jnp.log(0.5), jnp.log(2.5)))
    region = jnp.arange(TOKENS, dtype=jnp.int32) * 16 // TOKENS
    base = base * region_scale[region][:, None]
    return base.astype(jnp.bfloat16)


def level_of(stream_key, shape, cuts, low, largest):
    level, own = 1.0, jax.random.fold_in(stream_key, 6)
    for position, parts in cuts:
        heights = jnp.exp(jax.random.uniform(jax.random.fold_in(own, position), (parts,), jnp.float32, low / len(cuts), largest / len(cuts)))
        level = level * jnp.repeat(heights, shape[position] // parts).reshape([-1 if axis == position else 1 for axis in range(len(shape))])
    return level


def profile(number_of, total, bound, skew):
    weights = [(1 << 20) // math.isqrt(standing ** skew) + 1 for standing in range(2, number_of + 1)]
    spare, given = total - bound - (number_of - 1), [1] * (number_of - 1)
    while spare > 0:
        candidates = [i for i in range(number_of - 1) if given[i] < bound]
        pool, budget = sum([weights[i] for i in candidates]), spare
        for i in candidates:
            addition = min(bound - given[i], max(1, budget * weights[i] // pool), spare)
            given[i] = given[i] + addition
            spare = spare - addition
    return np.array([bound] + given)


def ragged_sizes(own_key, amount, total, limit, slope):
    if amount == 2:
        one = jax.random.randint(own_key, (), max(1, total - limit), min(limit, total - 1) + 1)
        return jnp.stack([one, total - one])
    lengths = jnp.asarray(profile(amount, total, limit, slope), jnp.int32)
    pairs = (amount - 1) // 2
    giver, receiver = lengths[1:1 + 2 * pairs:2], lengths[2:2 + 2 * pairs:2]
    margin = jnp.minimum(giver - 1, limit - receiver)
    shifted = jax.random.randint(jax.random.fold_in(own_key, 1), (pairs,), 0, 1 << 20) % (margin + 1)
    lengths = lengths.at[1:1 + 2 * pairs:2].set(giver - shifted).at[2:2 + 2 * pairs:2].set(receiver + shifted)
    return lengths[jax.random.permutation(jax.random.fold_in(own_key, 2), amount)]


def scatter_about(stream_key, extent, width, bound, shards=(), kind=jnp.bfloat16):
    values = jax.random.normal(stream_key, extent, jnp.float32) * width
    if len(shards) > 0:
        values = level_of(stream_key, extent, shards, -0.22, 0.18) * values
    return jnp.clip(values, min=-bound, max=bound).astype(kind)


def setup_inputs(seed: int = 0) -> dict:
    keys = jax.random.split(jax.random.key(seed), 9)
    return {
        "hidden": draw_hidden(jax.random.fold_in(keys[8], 71), 0),
        "w_query": scatter_about(keys[1], (D, HEADS * HEAD_DIM), D ** -0.5, 0.09375, ((1, 4),)),
        "w_key": scatter_about(keys[2], (D, KV_HEADS * HEAD_DIM), D ** -0.5, 0.09375, ((1, 4),)),
        "w_value": scatter_about(keys[3], (D, KV_HEADS * HEAD_DIM), D ** -0.5, 0.09375, ((1, 4),)),
        "cached_key": scatter_about(keys[4], (TOKENS, KV_HEADS * HEAD_DIM), 1.0, 6.0, ((0, 8), (1, 4))),
        "cached_value": scatter_about(keys[5], (TOKENS, KV_HEADS * HEAD_DIM), 1.0, 6.0, ((0, 8), (1, 4))),
        "doc_lengths": ragged_sizes(keys[6], DOCS, TOKENS, DOC_MOST, 2).astype(jnp.int32),
        "selected": draw_selected(jax.random.fold_in(keys[8], 71), 0),
    }


def doc_numbers(positions, doc_lengths):
    boundary = jnp.cumsum(doc_lengths).astype(jnp.int32)
    return jnp.sum((positions[:, None] >= boundary[None, :]).astype(jnp.int32), axis=1).astype(jnp.int32)


def reference(hidden, w_query, w_key, w_value, cached_key, cached_value, doc_lengths, selected):
    group_size = HEADS // KV_HEADS
    scaling = HEAD_DIM ** -0.5
    key_fresh = jnp.dot(hidden, w_key, preferred_element_type=jnp.float32)
    value_fresh = jnp.dot(hidden, w_value, preferred_element_type=jnp.float32)
    key_shift = key_fresh - cached_key.astype(jnp.float32)
    value_shift = value_fresh - cached_value.astype(jnp.float32)
    deviation = jnp.sum(key_shift * key_shift, axis=1) + jnp.sum(value_shift * value_shift, axis=1)
    positions = jnp.arange(TOKENS, dtype=jnp.int32)
    doc_of = doc_numbers(positions, doc_lengths)
    doc_table = (doc_of[:, None] == jnp.arange(DOCS, dtype=jnp.int32)[None, :]).astype(jnp.float32)
    doc_total = jnp.dot(deviation, doc_table, precision=lax.Precision.HIGHEST)
    doc_mean = doc_total / doc_lengths.astype(jnp.float32)
    score = deviation / (jnp.dot(doc_table, doc_mean, precision=lax.Precision.HIGHEST) + 1.0)
    picked = (jnp.arange(SELECTED, dtype=jnp.int32) // SEL_DEV) * TOK_DEV + selected.astype(jnp.int32)
    chosen = jnp.zeros((TOKENS,), jnp.int32).at[picked].set(1) > 0
    key_used = jnp.where(chosen[:, None], key_fresh.astype(jnp.bfloat16), cached_key)
    value_used = jnp.where(chosen[:, None], value_fresh.astype(jnp.bfloat16), cached_value)
    queries = jnp.dot(hidden[picked], w_query, preferred_element_type=jnp.float32).astype(jnp.bfloat16)
    allowed = positions[None, :] <= picked[:, None]
    query_heads = queries.astype(jnp.float32).reshape(SELECTED, HEADS, HEAD_DIM)

    def one_head(head_number):
        query_head = lax.dynamic_index_in_dim(query_heads, head_number, 1, keepdims=False)
        shared = (head_number // group_size).astype(jnp.int32)
        key_head = lax.dynamic_slice_in_dim(key_used, shared * HEAD_DIM, HEAD_DIM, 1).astype(jnp.float32)
        value_head = lax.dynamic_slice_in_dim(value_used, shared * HEAD_DIM, HEAD_DIM, 1).astype(jnp.float32)
        scores = jnp.dot(query_head, key_head.T, precision=lax.Precision.HIGHEST) * scaling
        scores = jnp.where(allowed, scores, -1e30)
        row_max = jnp.max(scores, axis=1, keepdims=True)
        weights = jnp.where(allowed, jnp.exp(scores - row_max), 0.0)
        row_sum = jnp.sum(weights, axis=1, keepdims=True)
        rounded = lax.optimization_barrier(weights.astype(jnp.bfloat16))
        mixed = jnp.dot(rounded.astype(jnp.float32), value_head, precision=lax.Precision.HIGHEST)
        return mixed / row_sum

    heads_out = lax.map(one_head, jnp.arange(HEADS, dtype=jnp.int32))
    attended = jnp.transpose(heads_out, (1, 0, 2)).reshape(SELECTED, HEADS * HEAD_DIM).astype(jnp.bfloat16)
    return attended, score
```

```python
import functools
import math

import jax
import jax.numpy as jnp
from jax import lax
from jax.experimental import pallas as pl
from jax.experimental.pallas import tpu as pltpu
from jax.sharding import PartitionSpec as P

HEADS = 32
KV_HEADS = 8
HEAD_DIM = 128
GROUP = HEADS // KV_HEADS
EXP_SCALE = HEAD_DIM ** (-0.5) * math.log2(math.e)
MESH = pl.DeviceIdType.MESH
NT = (((1,), (1,)), ((), ()))


def round_up(a, b):
    return -(-a // b) * b


def split_chips(chips):
    small = max(a for a in range(1, math.isqrt(chips) + 1) if chips % a == 0)
    return small, chips // small


def kernel(
    n, kz, docs, sel_rows,
    hid_hbm, wq_hbm, wk_hbm, wv_hbm, ck_hbm, cv_hbm, lens_ref, sel_ref,
    out_ref, score_ref,
    hid, wq, wk, wv, ck, cv, kbuf, vbuf, fresh, hq, q_ref, m_ref, l_ref, acc_ref, dev_ref, bias_ref,
    devbuf, docbuf,
    load_sem, own_send, fwd_send, relay_send, z_send, doc_send, recv, z_recv, doc_recv,
):
    tok = hid.shape[0]
    width = hid.shape[1]
    cols = wk.shape[1]
    local_heads = cols // HEAD_DIM
    pad = round_up(sel_rows, 16)
    qrows = GROUP * pad
    plain = tok - sel_rows
    cut = plain // 16 * 16
    parts = ((0, cut), (cut, tok - cut))
    bufs = (kbuf, vbuf)
    rows_a, rows_b = split_chips(n // 2)
    me = lax.axis_index("seq")
    zme = lax.axis_index("kvh")
    core = me % 2
    xx = (me // 2) % rows_b
    yy = me // (2 * rows_b)
    partner = me + 1 - 2 * core

    def at(dy, dx, dc=0):
        y = (yy + dy) % rows_a
        x = (xx + dx) % rows_b
        return (y * rows_b + x) * 2 + (core + dc) % 2

    half = tok // 2
    loads = [
        pltpu.make_async_copy(ck_hbm, ck, load_sem.at[0]),
        pltpu.make_async_copy(cv_hbm, cv, load_sem.at[1]),
        pltpu.make_async_copy(wk_hbm, wk, load_sem.at[2]),
        pltpu.make_async_copy(hid_hbm.at[pl.ds(0, half)], hid.at[pl.ds(0, half)], load_sem.at[3]),
        pltpu.make_async_copy(wv_hbm, wv, load_sem.at[4]),
        pltpu.make_async_copy(hid_hbm.at[pl.ds(half, half)], hid.at[pl.ds(half, half)], load_sem.at[5]),
        pltpu.make_async_copy(wq_hbm, wq, load_sem.at[6]),
    ]
    for load in loads:
        load.start()

    barrier = pltpu.get_barrier_semaphore()
    for d in range(1, n):
        pl.semaphore_signal(barrier, inc=1, device_id={"seq": (me + d) % n}, device_id_type=MESH)
    for d in range(1, kz):
        pl.semaphore_signal(barrier, inc=1, device_id={"kvh": (zme + d) % kz}, device_id_type=MESH)

    lane = lax.broadcasted_iota(jnp.int32, (8, tok), 1)

    def mark(r, chosen):
        return jnp.where(lane == sel_ref[me * sel_rows + r], 1, chosen)

    chosen = lax.fori_loop(0, sel_rows, mark, jnp.zeros((8, tok), jnp.int32), unroll=8)
    upper = (
        lax.broadcasted_iota(jnp.int32, (tok, tok), 0)
        <= lax.broadcasted_iota(jnp.int32, (tok, tok), 1)
    ).astype(jnp.float32).astype(jnp.bfloat16)
    count = jnp.dot(
        chosen.astype(jnp.float32).astype(jnp.bfloat16), upper, preferred_element_type=jnp.float32
    ).astype(jnp.int32)
    target = jnp.where(chosen > 0, plain + count - 1, lane - count)[0:1]

    def place(first, rows):
        row = lax.broadcasted_iota(jnp.int32, (rows, tok), 0) + first
        return (row == target).astype(jnp.float32).astype(jnp.bfloat16)

    first_place = place(0, cut)
    loads[0].wait()
    kbuf[me, 0:cut, :] = jnp.dot(first_place, ck[...], preferred_element_type=jnp.float32).astype(
        jnp.bfloat16
    )
    loads[1].wait()
    vbuf[me, 0:cut, :] = jnp.dot(first_place, cv[...], preferred_element_type=jnp.float32).astype(
        jnp.bfloat16
    )
    pl.semaphore_wait(barrier, n - 1 + kz - 1)

    def remote(src, arr, part, send_sem, dest):
        view = bufs[arr].at[src, pl.ds(parts[part][0], parts[part][1])]
        return pltpu.make_async_remote_copy(
            src_ref=view, dst_ref=view, send_sem=send_sem, recv_sem=recv.at[src, arr, part],
            device_id={"seq": dest}, device_id_type=MESH,
        )

    def whole(src, arr, send_sem):
        view = bufs[arr].at[src]
        return pltpu.make_async_remote_copy(
            src_ref=view, dst_ref=view, send_sem=send_sem, recv_sem=recv.at[src, arr, 0],
            device_id={"seq": partner}, device_id_type=MESH,
        )

    sends = []

    def send_own(part):
        for order in (0, 1):
            for d in range(1, rows_b):
                sends.append(remote(me, order, part, own_send.at[order, part, d - 1], at(0, d)))
                sends[-1].start()
            for d in range(1, rows_a):
                arr = 1 - order
                sends.append(
                    remote(me, arr, part, own_send.at[arr, part, rows_b - 1 + d - 1], at(d, 0))
                )
                sends[-1].start()

    def forward(part):
        for dx in range(1, rows_b):
            src = at(0, dx)
            remote(src, 0, part, own_send.at[0, part, 0], partner).wait_recv()
            for dy in range(1, rows_a):
                sem = fwd_send.at[0, part, (dx - 1) * (rows_a - 1) + dy - 1]
                sends.append(remote(src, 0, part, sem, at(dy, 0)))
                sends[-1].start()
        for dy in range(1, rows_a):
            src = at(dy, 0)
            remote(src, 1, part, own_send.at[0, part, 0], partner).wait_recv()
            for dx in range(1, rows_b):
                sem = fwd_send.at[1, part, (dx - 1) * (rows_a - 1) + dy - 1]
                sends.append(remote(src, 1, part, sem, at(0, dx)))
                sends[-1].start()

    send_own(0)

    loads[2].wait()
    for piece in range(2):
        rows = pl.ds(piece * half, half)
        loads[3 + 2 * piece].wait()
        key_fresh = jnp.dot(hid[rows, :], wk[...], preferred_element_type=jnp.float32)
        fresh[0, rows, :] = key_fresh.astype(jnp.bfloat16)
        key_shift = key_fresh - ck[rows, :].astype(jnp.float32)
        square = key_shift * key_shift
        if piece == 0:
            loads[4].wait()
        value_fresh = jnp.dot(hid[rows, :], wv[...], preferred_element_type=jnp.float32)
        fresh[1, rows, :] = value_fresh.astype(jnp.bfloat16)
        value_shift = value_fresh - cv[rows, :].astype(jnp.float32)
        square = square + value_shift * value_shift
        folded = square[:, 0:HEAD_DIM]
        for h in range(1, local_heads):
            folded = folded + square[:, h * HEAD_DIM:(h + 1) * HEAD_DIM]
        total = jnp.sum(folded.T, axis=0, keepdims=True)
        dev_ref[:, piece * half:(piece + 1) * half] = jnp.broadcast_to(total, (8, half))

    last_row = lax.broadcasted_iota(jnp.int32, (tok - cut, tok), 0) + cut
    hit = last_row == target
    old = jnp.where(hit & (last_row < plain), 1.0, 0.0).astype(jnp.bfloat16)
    new = jnp.where(hit & (last_row >= plain), 1.0, 0.0).astype(jnp.bfloat16)
    for arr, cached in enumerate((ck, cv)):
        tail = jnp.dot(old, cached[...], preferred_element_type=jnp.float32)
        tail = tail + jnp.dot(new, fresh[arr], preferred_element_type=jnp.float32)
        bufs[arr][me, cut:tok, :] = tail.astype(jnp.bfloat16)
    devbuf[zme] = dev_ref[...]
    forward(0)
    send_own(1)
    relays = [whole(me, arr, relay_send.at[0, arr]) for arr in (0, 1)]
    for relay in relays:
        relay.start()
    for d in range(1, kz):
        sends.append(
            pltpu.make_async_remote_copy(
                src_ref=devbuf.at[zme], dst_ref=devbuf.at[zme], send_sem=z_send.at[d - 1],
                recv_sem=z_recv.at[zme], device_id={"kvh": (zme + d) % kz}, device_id_type=MESH,
            )
        )
        sends[-1].start()

    pick = place(plain, pad)
    step = width // 4
    for c in range(4):
        chunk = slice(c * step, (c + 1) * step)
        hq[:, chunk] = jnp.dot(pick, hid[:, chunk], preferred_element_type=jnp.float32).astype(
            jnp.bfloat16
        )
    loads[6].wait()

    def project(h, carry):
        chunk = pl.ds(pl.multiple_of(h * GROUP * HEAD_DIM, HEAD_DIM), GROUP * HEAD_DIM)
        queries = jnp.dot(hq[...], wq[:, chunk], preferred_element_type=jnp.float32).astype(
            jnp.bfloat16
        )
        for g in range(GROUP):
            q_ref[h, g * pad:(g + 1) * pad, :] = queries[:, g * HEAD_DIM:(g + 1) * HEAD_DIM]
        return carry

    lax.fori_loop(0, local_heads, project, 0)

    forward(1)
    code = jnp.where(
        lax.broadcasted_iota(jnp.int32, (8, tok), 0) == 0, lane % 256, lane // 256
    ).astype(jnp.float32).astype(jnp.bfloat16)
    found = lax.dot_general(code, place(0, tok), NT, preferred_element_type=jnp.float32)
    key_pos = (found[0:1] + 256.0 * found[1:2]).astype(jnp.int32)
    pad_lane = lax.broadcasted_iota(jnp.int32, (pad, tok), 1)
    row_pos = jnp.sum(
        jnp.where(pick.astype(jnp.float32) > 0, pad_lane.astype(jnp.float32), 0.0),
        axis=1, keepdims=True,
    ).astype(jnp.int32)
    bias_ref[...] = jnp.where(key_pos <= row_pos, 0.0, -1e30)

    chunks = 2
    crows = qrows // chunks

    def attend(src, h, c, own):
        rows = pl.ds(pl.multiple_of(c * crows, 16), crows)
        head = pl.ds(pl.multiple_of(h * HEAD_DIM, HEAD_DIM), HEAD_DIM)
        scores = lax.dot_general(
            q_ref[h, rows, :], kbuf[src, :, head], NT, preferred_element_type=jnp.float32
        )
        if own:
            scores = scores + jnp.concatenate([bias_ref[...]] * (crows // pad), axis=0)
        best = jnp.max(scores, axis=1, keepdims=True)
        if not own:
            before = m_ref[h, rows, :]
            best = jnp.maximum(best, before)
        weights = jnp.exp2((scores - best) * EXP_SCALE)
        row_sum = jnp.sum(weights, axis=1, keepdims=True)
        mixed = jnp.dot(
            weights.astype(jnp.bfloat16), vbuf[src, :, head], preferred_element_type=jnp.float32
        )
        if not own:
            fade = jnp.exp2((before - best) * EXP_SCALE)
            row_sum = row_sum + l_ref[h, rows, :] * fade
            mixed = mixed + acc_ref[h, rows, :] * fade
        m_ref[h, rows, :] = best
        l_ref[h, rows, :] = row_sum
        acc_ref[h, rows, :] = mixed

    def attend_all(src, own):
        def one(i, carry):
            attend(src, i // chunks, i % chunks, own)
            return carry

        lax.fori_loop(0, local_heads * chunks, one, 0)

    attend_all(me, True)

    for d in range(1, kz):
        src = (zme + d) % kz
        pltpu.make_async_remote_copy(
            src_ref=devbuf.at[src], dst_ref=devbuf.at[src], send_sem=z_send.at[0],
            recv_sem=z_recv.at[src], device_id={"kvh": src}, device_id_type=MESH,
        ).wait_recv()
    deviation = devbuf[0]
    for z in range(1, kz):
        deviation = deviation + devbuf[z]
    deviation = deviation[0:1]
    position = lane[0:1] + me * tok
    inside = []
    end = jnp.int32(0)
    for d in range(docs):
        begin, end = end, end + lens_ref[d]
        inside.append((position >= begin) & (position < end))
    slot_row = lax.broadcasted_iota(jnp.int32, docbuf.shape[1:], 0)
    shares = jnp.zeros(docbuf.shape[1:], jnp.float32)
    for d in range(docs):
        share = jnp.sum(jnp.where(inside[d], deviation, 0.0), axis=1, keepdims=True)
        shares = jnp.where(slot_row == d, share, shares)
    docbuf[me] = shares
    for d in range(1, n):
        sends.append(
            pltpu.make_async_remote_copy(
                src_ref=docbuf.at[me], dst_ref=docbuf.at[me], send_sem=doc_send.at[d - 1],
                recv_sem=doc_recv.at[me], device_id={"seq": (me + d) % n}, device_id_type=MESH,
            )
        )
        sends[-1].start()

    def other(s, carry):
        dc = s % 2
        dx = (s // 2) % rows_b
        dy = s // (2 * rows_b)
        src = at(dy, dx, dc)

        @pl.when(dc == 1)
        def _():
            for arr in (0, 1):
                whole(src, arr, relay_send.at[0, arr]).wait_recv()

        @pl.when(dc == 0)
        def _():
            @pl.when(dy != 0)
            def _():
                for part in (0, 1):
                    remote(src, 0, part, own_send.at[0, part, 0], partner).wait_recv()

            @pl.when(dx != 0)
            def _():
                for part in (0, 1):
                    remote(src, 1, part, own_send.at[0, part, 0], partner).wait_recv()

            for arr in (0, 1):
                whole(src, arr, relay_send.at[s // 2, arr]).start()

        @pl.when(src < me)
        def _():
            attend_all(src, False)

        return carry

    lax.fori_loop(1, n, other, 0)

    for h in range(local_heads):
        done = (acc_ref[h] / l_ref[h]).astype(jnp.bfloat16)
        for g in range(GROUP):
            head = h * GROUP + g
            out_ref[:, head * HEAD_DIM:(head + 1) * HEAD_DIM] = done[g * pad:g * pad + sel_rows]

    for d in range(1, n):
        src = (me + d) % n
        pltpu.make_async_remote_copy(
            src_ref=docbuf.at[src], dst_ref=docbuf.at[src], send_sem=doc_send.at[0],
            recv_sem=doc_recv.at[src], device_id={"seq": src}, device_id_type=MESH,
        ).wait_recv()
    totals = docbuf[0]
    for s in range(1, n):
        totals = totals + docbuf[s]
    mean = jnp.zeros((1, tok), jnp.float32)
    for d in range(docs):
        here = totals[d:d + 1, 0:1] / lens_ref[d].astype(jnp.float32)
        mean = jnp.where(inside[d], here, mean)
    score_ref[...] = deviation / (mean + 1.0)

    for send in sends:
        send.wait_send()

    def drain(s, carry):
        for arr in (0, 1):
            whole(me, arr, relay_send.at[s, arr]).wait_send()
        return carry

    lax.fori_loop(0, n // 2, drain, 0)


def shards(n, kz, hidden, w_query, w_key, w_value, cached_key, cached_value, doc_lengths, selected):
    tok, width = hidden.shape
    cols = w_key.shape[1]
    qcols = w_query.shape[1]
    sel_rows = selected.shape[0] // n
    docs = doc_lengths.shape[0]
    pad = round_up(sel_rows, 16)
    local_heads = cols // HEAD_DIM
    qrows = GROUP * pad
    rows_a, rows_b = split_chips(n // 2)
    peers = max(1, rows_a + rows_b - 2)
    forwards = max(1, (rows_a - 1) * (rows_b - 1))
    bf, f32 = jnp.bfloat16, jnp.float32
    dma = pltpu.SemaphoreType.DMA
    any_space = pl.BlockSpec(memory_space=pl.ANY)
    vmem = pl.BlockSpec(memory_space=pltpu.VMEM)
    smem = pl.BlockSpec(memory_space=pltpu.SMEM)
    attended, score = pl.pallas_call(
        functools.partial(kernel, n, kz, docs, sel_rows),
        out_shape=(
            jax.ShapeDtypeStruct((sel_rows, qcols), bf),
            jax.ShapeDtypeStruct((1, tok), f32),
        ),
        in_specs=[any_space] * 6 + [smem] * 2,
        out_specs=(vmem, vmem),
        scratch_shapes=[
            pltpu.VMEM((tok, width), bf),
            pltpu.VMEM((width, qcols), bf),
            pltpu.VMEM((width, cols), bf),
            pltpu.VMEM((width, cols), bf),
            pltpu.VMEM((tok, cols), bf),
            pltpu.VMEM((tok, cols), bf),
            pltpu.VMEM((n, tok, cols), bf),
            pltpu.VMEM((n, tok, cols), bf),
            pltpu.VMEM((2, tok, cols), bf),
            pltpu.VMEM((pad, width), bf),
            pltpu.VMEM((local_heads, qrows, HEAD_DIM), bf),
            pltpu.VMEM((local_heads, qrows, 1), f32),
            pltpu.VMEM((local_heads, qrows, 1), f32),
            pltpu.VMEM((local_heads, qrows, HEAD_DIM), f32),
            pltpu.VMEM((8, tok), f32),
            pltpu.VMEM((pad, tok), f32),
            pltpu.VMEM((kz, 8, tok), f32),
            pltpu.VMEM((n, round_up(docs, 8), 128), f32),
            dma((7,)),
            dma((2, 2, peers)),
            dma((2, 2, forwards)),
            dma((n // 2, 2)),
            dma((max(1, kz - 1),)),
            dma((n - 1,)),
            dma((n, 2, 2)),
            dma((kz,)),
            dma((n,)),
        ],
        compiler_params=pltpu.CompilerParams(
            collective_id=0, has_side_effects=True, vmem_limit_bytes=62 * 1024 * 1024
        ),
        name="blend",
    )(hidden, w_query, w_key, w_value, cached_key, cached_value, doc_lengths, selected)
    return attended, score.reshape(tok)


def solution(mesh):
    return jax.shard_map(
        functools.partial(shards, mesh.shape["seq"], mesh.shape["kvh"]),
        mesh=mesh,
        in_specs=(
            P("seq", None),
            P(None, "kvh"),
            P(None, "kvh"),
            P(None, "kvh"),
            P("seq", "kvh"),
            P("seq", "kvh"),
            P(),
            P(),
        ),
        out_specs=(P("seq", "kvh"), P("seq")),
        check_vma=False,
    )
```

```python
import functools
import math

import jax
import jax.numpy as jnp
from jax import lax
from jax.experimental import pallas as pl
from jax.experimental.pallas import tpu as pltpu
from jax.sharding import PartitionSpec as P

HEADS = 32
KV_HEADS = 8
HEAD_DIM = 128
GROUP = HEADS // KV_HEADS
EXP_SCALE = HEAD_DIM ** (-0.5) * math.log2(math.e)
MESH = pl.DeviceIdType.MESH
NT = (((1,), (1,)), ((), ()))


def round_up(a, b):
    return -(-a // b) * b


def split_chips(chips):
    small = max(a for a in range(1, math.isqrt(chips) + 1) if chips % a == 0)
    return small, chips // small


def kernel(
    n, kz, docs, sel_rows,
    hid_hbm, wq_hbm, wk_hbm, wv_hbm, ck_hbm, cv_hbm, lens_ref, sel_ref,
    out_ref, score_ref,
    hid, wq, wk, wv, ck, cv, kbuf, vbuf, fresh, hq, q_ref, m_ref, l_ref, acc_ref, dev_ref, bias_ref,
    devbuf, docbuf,
    load_sem, own_send, fwd_send, relay_send, z_send, doc_send, recv, z_recv, doc_recv,
):
    tok = hid.shape[0]
    width = hid.shape[1]
    cols = wk.shape[1]
    local_heads = cols // HEAD_DIM
    pad = round_up(sel_rows, 16)
    qrows = GROUP * pad
    plain = tok - sel_rows
    cut = plain // 16 * 16
    parts = ((0, cut), (cut, tok - cut))
    bufs = (kbuf, vbuf)
    rows_a, rows_b = split_chips(n // 2)
    me = lax.axis_index("seq")
    zme = lax.axis_index("kvh")
    core = me % 2
    xx = (me // 2) % rows_b
    yy = me // (2 * rows_b)
    partner = me + 1 - 2 * core

    def at(dy, dx, dc=0):
        y = (yy + dy) % rows_a
        x = (xx + dx) % rows_b
        return (y * rows_b + x) * 2 + (core + dc) % 2

    half = tok // 2
    loads = [
        pltpu.make_async_copy(ck_hbm, ck, load_sem.at[0]),
        pltpu.make_async_copy(cv_hbm, cv, load_sem.at[1]),
        pltpu.make_async_copy(wk_hbm, wk, load_sem.at[2]),
        pltpu.make_async_copy(hid_hbm.at[pl.ds(0, half)], hid.at[pl.ds(0, half)], load_sem.at[3]),
        pltpu.make_async_copy(wv_hbm, wv, load_sem.at[4]),
        pltpu.make_async_copy(hid_hbm.at[pl.ds(half, half)], hid.at[pl.ds(half, half)], load_sem.at[5]),
        pltpu.make_async_copy(wq_hbm, wq, load_sem.at[6]),
    ]
    for load in loads:
        load.start()

    barrier = pltpu.get_barrier_semaphore()
    for d in range(1, n):
        pl.semaphore_signal(barrier, inc=1, device_id={"seq": (me + d) % n}, device_id_type=MESH)
    for d in range(1, kz):
        pl.semaphore_signal(barrier, inc=1, device_id={"kvh": (zme + d) % kz}, device_id_type=MESH)

    lane = lax.broadcasted_iota(jnp.int32, (8, tok), 1)

    def mark(r, chosen):
        return jnp.where(lane == sel_ref[me * sel_rows + r], 1, chosen)

    chosen = lax.fori_loop(0, sel_rows, mark, jnp.zeros((8, tok), jnp.int32), unroll=8)
    upper = (
        lax.broadcasted_iota(jnp.int32, (tok, tok), 0)
        <= lax.broadcasted_iota(jnp.int32, (tok, tok), 1)
    ).astype(jnp.float32).astype(jnp.bfloat16)
    count = jnp.dot(
        chosen.astype(jnp.float32).astype(jnp.bfloat16), upper, preferred_element_type=jnp.float32
    ).astype(jnp.int32)
    target = jnp.where(chosen > 0, plain + count - 1, lane - count)[0:1]

    def place(first, rows):
        row = lax.broadcasted_iota(jnp.int32, (rows, tok), 0) + first
        return (row == target).astype(jnp.float32).astype(jnp.bfloat16)

    first_place = place(0, cut)
    loads[0].wait()
    kbuf[me, 0:cut, :] = jnp.dot(first_place, ck[...], preferred_element_type=jnp.float32).astype(
        jnp.bfloat16
    )
    loads[1].wait()
    vbuf[me, 0:cut, :] = jnp.dot(first_place, cv[...], preferred_element_type=jnp.float32).astype(
        jnp.bfloat16
    )
    pl.semaphore_wait(barrier, n - 1 + kz - 1)

    def remote(src, arr, part, send_sem, dest):
        view = bufs[arr].at[src, pl.ds(parts[part][0], parts[part][1])]
        return pltpu.make_async_remote_copy(
            src_ref=view, dst_ref=view, send_sem=send_sem, recv_sem=recv.at[src, arr, part],
            device_id={"seq": dest}, device_id_type=MESH,
        )

    sends = []

    def relay(src, s, part):
        for arr in (0, 1):
            remote(src, arr, part, relay_send.at[s, arr, part], partner).start()

    def send_own(part):
        relay(me, 0, part)
        for order in (0, 1):
            for d in range(1, rows_b):
                sends.append(remote(me, order, part, own_send.at[order, part, d - 1], at(0, d)))
                sends[-1].start()
            for d in range(1, rows_a):
                arr = 1 - order
                sends.append(
                    remote(me, arr, part, own_send.at[arr, part, rows_b - 1 + d - 1], at(d, 0))
                )
                sends[-1].start()

    def forward(part):
        for dx in range(1, rows_b):
            src = at(0, dx)
            remote(src, 0, part, own_send.at[0, part, 0], partner).wait_recv()
            for dy in range(1, rows_a):
                sem = fwd_send.at[0, part, (dx - 1) * (rows_a - 1) + dy - 1]
                sends.append(remote(src, 0, part, sem, at(dy, 0)))
                sends[-1].start()
        for dy in range(1, rows_a):
            src = at(dy, 0)
            remote(src, 1, part, own_send.at[0, part, 0], partner).wait_recv()
            for dx in range(1, rows_b):
                sem = fwd_send.at[1, part, (dx - 1) * (rows_a - 1) + dy - 1]
                sends.append(remote(src, 1, part, sem, at(0, dx)))
                sends[-1].start()

    send_own(0)

    loads[2].wait()
    for piece in range(2):
        rows = pl.ds(piece * half, half)
        loads[3 + 2 * piece].wait()
        key_fresh = jnp.dot(hid[rows, :], wk[...], preferred_element_type=jnp.float32)
        fresh[0, rows, :] = key_fresh.astype(jnp.bfloat16)
        key_shift = key_fresh - ck[rows, :].astype(jnp.float32)
        square = key_shift * key_shift
        if piece == 0:
            loads[4].wait()
        value_fresh = jnp.dot(hid[rows, :], wv[...], preferred_element_type=jnp.float32)
        fresh[1, rows, :] = value_fresh.astype(jnp.bfloat16)
        value_shift = value_fresh - cv[rows, :].astype(jnp.float32)
        square = square + value_shift * value_shift
        folded = square[:, 0:HEAD_DIM]
        for h in range(1, local_heads):
            folded = folded + square[:, h * HEAD_DIM:(h + 1) * HEAD_DIM]
        total = jnp.sum(folded.T, axis=0, keepdims=True)
        dev_ref[:, piece * half:(piece + 1) * half] = jnp.broadcast_to(total, (8, half))

    last_row = lax.broadcasted_iota(jnp.int32, (tok - cut, tok), 0) + cut
    hit = last_row == target
    old = jnp.where(hit & (last_row < plain), 1.0, 0.0).astype(jnp.bfloat16)
    new = jnp.where(hit & (last_row >= plain), 1.0, 0.0).astype(jnp.bfloat16)
    for arr, cached in enumerate((ck, cv)):
        tail = jnp.dot(old, cached[...], preferred_element_type=jnp.float32)
        tail = tail + jnp.dot(new, fresh[arr], preferred_element_type=jnp.float32)
        bufs[arr][me, cut:tok, :] = tail.astype(jnp.bfloat16)
    devbuf[zme] = dev_ref[...]
    send_own(1)
    forward(0)
    for d in range(1, kz):
        sends.append(
            pltpu.make_async_remote_copy(
                src_ref=devbuf.at[zme], dst_ref=devbuf.at[zme], send_sem=z_send.at[d - 1],
                recv_sem=z_recv.at[zme], device_id={"kvh": (zme + d) % kz}, device_id_type=MESH,
            )
        )
        sends[-1].start()

    pick = place(plain, pad)
    step = width // 4
    for c in range(4):
        chunk = slice(c * step, (c + 1) * step)
        hq[:, chunk] = jnp.dot(pick, hid[:, chunk], preferred_element_type=jnp.float32).astype(
            jnp.bfloat16
        )
    loads[6].wait()

    def project(h, carry):
        chunk = pl.ds(pl.multiple_of(h * GROUP * HEAD_DIM, HEAD_DIM), GROUP * HEAD_DIM)
        queries = jnp.dot(hq[...], wq[:, chunk], preferred_element_type=jnp.float32).astype(
            jnp.bfloat16
        )
        for g in range(GROUP):
            q_ref[h, g * pad:(g + 1) * pad, :] = queries[:, g * HEAD_DIM:(g + 1) * HEAD_DIM]
        return carry

    lax.fori_loop(0, local_heads, project, 0)

    code = jnp.where(
        lax.broadcasted_iota(jnp.int32, (8, tok), 0) == 0, lane % 256, lane // 256
    ).astype(jnp.float32).astype(jnp.bfloat16)
    found = lax.dot_general(code, place(0, tok), NT, preferred_element_type=jnp.float32)
    key_pos = (found[0:1] + 256.0 * found[1:2]).astype(jnp.int32)
    pad_lane = lax.broadcasted_iota(jnp.int32, (pad, tok), 1)
    row_pos = jnp.sum(
        jnp.where(pick.astype(jnp.float32) > 0, pad_lane.astype(jnp.float32), 0.0),
        axis=1, keepdims=True,
    ).astype(jnp.int32)
    bias_ref[...] = jnp.where(key_pos <= row_pos, 0.0, -1e30)

    chunks = 2
    crows = qrows // chunks

    def attend(src, h, c, keys, own):
        rows = slice(c * crows, (c + 1) * crows)
        head = slice(h * HEAD_DIM, (h + 1) * HEAD_DIM)
        scores = lax.dot_general(
            q_ref[h, rows, :], kbuf[src, keys, head], NT, preferred_element_type=jnp.float32
        )
        if own:
            scores = scores + jnp.concatenate([bias_ref[...]] * (crows // pad), axis=0)
        best = jnp.max(scores, axis=1, keepdims=True)
        if not own:
            before = m_ref[h, rows, :]
            best = jnp.maximum(best, before)
        weights = jnp.exp2((scores - best) * EXP_SCALE)
        row_sum = jnp.sum(weights, axis=1, keepdims=True)
        mixed = jnp.dot(
            weights.astype(jnp.bfloat16), vbuf[src, keys, head], preferred_element_type=jnp.float32
        )
        if not own:
            fade = jnp.exp2((before - best) * EXP_SCALE)
            row_sum = row_sum + l_ref[h, rows, :] * fade
            mixed = mixed + acc_ref[h, rows, :] * fade
        m_ref[h, rows, :] = best
        l_ref[h, rows, :] = row_sum
        acc_ref[h, rows, :] = mixed

    def attend_all(src, first, count, own):
        for h in range(local_heads):
            for c in range(chunks):
                attend(src, h, c, slice(first, first + count), own)

    attend_all(me, 0, tok, True)

    for d in range(1, kz):
        src = (zme + d) % kz
        pltpu.make_async_remote_copy(
            src_ref=devbuf.at[src], dst_ref=devbuf.at[src], send_sem=z_send.at[0],
            recv_sem=z_recv.at[src], device_id={"kvh": src}, device_id_type=MESH,
        ).wait_recv()
    deviation = devbuf[0]
    for z in range(1, kz):
        deviation = deviation + devbuf[z]
    deviation = deviation[0:1]
    position = lane[0:1] + me * tok
    inside = []
    end = jnp.int32(0)
    for d in range(docs):
        begin, end = end, end + lens_ref[d]
        inside.append((position >= begin) & (position < end))
    slot_row = lax.broadcasted_iota(jnp.int32, docbuf.shape[1:], 0)
    shares = jnp.zeros(docbuf.shape[1:], jnp.float32)
    for d in range(docs):
        share = jnp.sum(jnp.where(inside[d], deviation, 0.0), axis=1, keepdims=True)
        shares = jnp.where(slot_row == d, share, shares)
    docbuf[me] = shares
    for d in range(1, n):
        sends.append(
            pltpu.make_async_remote_copy(
                src_ref=docbuf.at[me], dst_ref=docbuf.at[me], send_sem=doc_send.at[d - 1],
                recv_sem=doc_recv.at[me], device_id={"seq": (me + d) % n}, device_id_type=MESH,
            )
        )
        sends[-1].start()

    def other(part, s, carry):
        dc = s % 2
        dx = (s // 2) % rows_b
        dy = s // (2 * rows_b)
        src = at(dy, dx, dc)
        idle = own_send.at[0, part, 0]

        @pl.when((dc == 1) | (dy != 0))
        def _():
            remote(src, 0, part, idle, partner).wait_recv()

        @pl.when((dc == 1) | (dx != 0))
        def _():
            remote(src, 1, part, idle, partner).wait_recv()

        @pl.when(dc == 0)
        def _():
            relay(src, s // 2, part)

        @pl.when(src < me)
        def _():
            attend_all(src, *parts[part], False)

        return carry

    lax.fori_loop(1, n - 2, functools.partial(other, 0), 0)
    forward(1)
    lax.fori_loop(n - 2, n, functools.partial(other, 0), 0)
    lax.fori_loop(1, n, functools.partial(other, 1), 0)

    for h in range(local_heads):
        done = (acc_ref[h] / l_ref[h]).astype(jnp.bfloat16)
        for g in range(GROUP):
            head = h * GROUP + g
            out_ref[:, head * HEAD_DIM:(head + 1) * HEAD_DIM] = done[g * pad:g * pad + sel_rows]

    for d in range(1, n):
        src = (me + d) % n
        pltpu.make_async_remote_copy(
            src_ref=docbuf.at[src], dst_ref=docbuf.at[src], send_sem=doc_send.at[0],
            recv_sem=doc_recv.at[src], device_id={"seq": src}, device_id_type=MESH,
        ).wait_recv()
    totals = docbuf[0]
    for s in range(1, n):
        totals = totals + docbuf[s]
    mean = jnp.zeros((1, tok), jnp.float32)
    for d in range(docs):
        here = totals[d:d + 1, 0:1] / lens_ref[d].astype(jnp.float32)
        mean = jnp.where(inside[d], here, mean)
    score_ref[...] = deviation / (mean + 1.0)

    for send in sends:
        send.wait_send()

    def drain(s, carry):
        for part in (0, 1):
            for arr in (0, 1):
                remote(me, arr, part, relay_send.at[s, arr, part], partner).wait_send()
        return carry

    lax.fori_loop(0, n // 2, drain, 0)


def shards(n, kz, hidden, w_query, w_key, w_value, cached_key, cached_value, doc_lengths, selected):
    tok, width = hidden.shape
    cols = w_key.shape[1]
    qcols = w_query.shape[1]
    sel_rows = selected.shape[0] // n
    docs = doc_lengths.shape[0]
    pad = round_up(sel_rows, 16)
    local_heads = cols // HEAD_DIM
    qrows = GROUP * pad
    rows_a, rows_b = split_chips(n // 2)
    peers = max(1, rows_a + rows_b - 2)
    forwards = max(1, (rows_a - 1) * (rows_b - 1))
    bf, f32 = jnp.bfloat16, jnp.float32
    dma = pltpu.SemaphoreType.DMA
    any_space = pl.BlockSpec(memory_space=pl.ANY)
    vmem = pl.BlockSpec(memory_space=pltpu.VMEM)
    smem = pl.BlockSpec(memory_space=pltpu.SMEM)
    attended, score = pl.pallas_call(
        functools.partial(kernel, n, kz, docs, sel_rows),
        out_shape=(
            jax.ShapeDtypeStruct((sel_rows, qcols), bf),
            jax.ShapeDtypeStruct((1, tok), f32),
        ),
        in_specs=[any_space] * 6 + [smem] * 2,
        out_specs=(vmem, vmem),
        scratch_shapes=[
            pltpu.VMEM((tok, width), bf),
            pltpu.VMEM((width, qcols), bf),
            pltpu.VMEM((width, cols), bf),
            pltpu.VMEM((width, cols), bf),
            pltpu.VMEM((tok, cols), bf),
            pltpu.VMEM((tok, cols), bf),
            pltpu.VMEM((n, tok, cols), bf),
            pltpu.VMEM((n, tok, cols), bf),
            pltpu.VMEM((2, tok, cols), bf),
            pltpu.VMEM((pad, width), bf),
            pltpu.VMEM((local_heads, qrows, HEAD_DIM), bf),
            pltpu.VMEM((local_heads, qrows, 1), f32),
            pltpu.VMEM((local_heads, qrows, 1), f32),
            pltpu.VMEM((local_heads, qrows, HEAD_DIM), f32),
            pltpu.VMEM((8, tok), f32),
            pltpu.VMEM((pad, tok), f32),
            pltpu.VMEM((kz, 8, tok), f32),
            pltpu.VMEM((n, round_up(docs, 8), 128), f32),
            dma((7,)),
            dma((2, 2, peers)),
            dma((2, 2, forwards)),
            dma((n // 2, 2, 2)),
            dma((max(1, kz - 1),)),
            dma((n - 1,)),
            dma((n, 2, 2)),
            dma((kz,)),
            dma((n,)),
        ],
        compiler_params=pltpu.CompilerParams(
            collective_id=0, has_side_effects=True, vmem_limit_bytes=62 * 1024 * 1024
        ),
        name="blend",
    )(hidden, w_query, w_key, w_value, cached_key, cached_value, doc_lengths, selected)
    return attended, score.reshape(tok)


def solution(mesh):
    return jax.shard_map(
        functools.partial(shards, mesh.shape["seq"], mesh.shape["kvh"]),
        mesh=mesh,
        in_specs=(
            P("seq", None),
            P(None, "kvh"),
            P(None, "kvh"),
            P(None, "kvh"),
            P("seq", "kvh"),
            P("seq", "kvh"),
            P(),
            P(),
        ),
        out_specs=(P("seq", "kvh"), P("seq")),
        check_vma=False,
    )
```

```python
import functools
import math

import jax
import jax.numpy as jnp
from jax import lax
from jax.experimental import pallas as pl
from jax.experimental.pallas import tpu as pltpu
from jax.sharding import PartitionSpec as P

HEADS = 32
KV_HEADS = 8
HEAD_DIM = 128
GROUP = HEADS // KV_HEADS
EXP_SCALE = HEAD_DIM ** (-0.5) * math.log2(math.e)
MESH = pl.DeviceIdType.MESH
NT = (((1,), (1,)), ((), ()))


def round_up(a, b):
    return -(-a // b) * b


def split_chips(chips):
    small = max(a for a in range(1, math.isqrt(chips) + 1) if chips % a == 0)
    return small, chips // small


def kernel(
    n, kz, docs, sel_rows,
    hid_hbm, wq_hbm, wk_hbm, wv_hbm, ck_hbm, cv_hbm, lens_ref, sel_ref,
    out_ref, score_ref,
    hid, wq, wk, wv, ck, cv, kbuf, vbuf, fresh, hq, q_ref, m_ref, l_ref, acc_ref, dev_ref, bias_ref,
    devbuf, docbuf,
    load_sem, own_send, fwd_send, relay_send, z_send, doc_send, recv, z_recv, doc_recv,
):
    tok = hid.shape[0]
    width = hid.shape[1]
    cols = wk.shape[1]
    local_heads = cols // HEAD_DIM
    pad = round_up(sel_rows, 16)
    qrows = GROUP * pad
    plain = tok - sel_rows
    cut = plain // 16 * 16
    parts = ((0, cut), (cut, tok - cut))
    bufs = (kbuf, vbuf)
    rows_a, rows_b = split_chips(n // 2)
    me = lax.axis_index("seq")
    zme = lax.axis_index("kvh")
    core = me % 2
    xx = (me // 2) % rows_b
    yy = me // (2 * rows_b)
    partner = me + 1 - 2 * core

    def at(dy, dx, dc=0):
        y = (yy + dy) % rows_a
        x = (xx + dx) % rows_b
        return (y * rows_b + x) * 2 + (core + dc) % 2

    half = tok // 2
    loads = [
        pltpu.make_async_copy(ck_hbm, ck, load_sem.at[0]),
        pltpu.make_async_copy(cv_hbm, cv, load_sem.at[1]),
        pltpu.make_async_copy(wk_hbm, wk, load_sem.at[2]),
        pltpu.make_async_copy(hid_hbm.at[pl.ds(0, half)], hid.at[pl.ds(0, half)], load_sem.at[3]),
        pltpu.make_async_copy(wv_hbm, wv, load_sem.at[4]),
        pltpu.make_async_copy(hid_hbm.at[pl.ds(half, half)], hid.at[pl.ds(half, half)], load_sem.at[5]),
        pltpu.make_async_copy(wq_hbm, wq, load_sem.at[6]),
    ]
    for load in loads:
        load.start()

    barrier = pltpu.get_barrier_semaphore()
    for d in range(1, n):
        pl.semaphore_signal(barrier, inc=1, device_id={"seq": (me + d) % n}, device_id_type=MESH)
    for d in range(1, kz):
        pl.semaphore_signal(barrier, inc=1, device_id={"kvh": (zme + d) % kz}, device_id_type=MESH)

    lane = lax.broadcasted_iota(jnp.int32, (8, tok), 1)

    def mark(r, chosen):
        return jnp.where(lane == sel_ref[me * sel_rows + r], 1, chosen)

    chosen = lax.fori_loop(0, sel_rows, mark, jnp.zeros((8, tok), jnp.int32), unroll=8)
    upper = (
        lax.broadcasted_iota(jnp.int32, (tok, tok), 0)
        <= lax.broadcasted_iota(jnp.int32, (tok, tok), 1)
    ).astype(jnp.float32).astype(jnp.bfloat16)
    count = jnp.dot(
        chosen.astype(jnp.float32).astype(jnp.bfloat16), upper, preferred_element_type=jnp.float32
    ).astype(jnp.int32)
    target = jnp.where(chosen > 0, plain + count - 1, lane - count)[0:1]

    def place(first, rows):
        row = lax.broadcasted_iota(jnp.int32, (rows, tok), 0) + first
        return (row == target).astype(jnp.float32).astype(jnp.bfloat16)

    first_place = place(0, cut)
    loads[0].wait()
    kbuf[me, 0:cut, :] = jnp.dot(first_place, ck[...], preferred_element_type=jnp.float32).astype(
        jnp.bfloat16
    )
    loads[1].wait()
    vbuf[me, 0:cut, :] = jnp.dot(first_place, cv[...], preferred_element_type=jnp.float32).astype(
        jnp.bfloat16
    )
    pl.semaphore_wait(barrier, n - 1 + kz - 1)

    def remote(src, arr, part, send_sem, dest):
        view = bufs[arr].at[src, pl.ds(parts[part][0], parts[part][1])]
        return pltpu.make_async_remote_copy(
            src_ref=view, dst_ref=view, send_sem=send_sem, recv_sem=recv.at[src, arr, part],
            device_id={"seq": dest}, device_id_type=MESH,
        )

    sends = []

    def relay(src, s, part):
        for arr in (0, 1):
            remote(src, arr, part, relay_send.at[s, arr, part], partner).start()

    def send_own(part):
        relay(me, 0, part)
        for order in (0, 1):
            for d in range(1, rows_b):
                sends.append(remote(me, order, part, own_send.at[order, part, d - 1], at(0, d)))
                sends[-1].start()
            for d in range(1, rows_a):
                arr = 1 - order
                sends.append(
                    remote(me, arr, part, own_send.at[arr, part, rows_b - 1 + d - 1], at(d, 0))
                )
                sends[-1].start()

    def forward(part):
        for dx in range(1, rows_b):
            src = at(0, dx)
            remote(src, 0, part, own_send.at[0, part, 0], partner).wait_recv()
            for dy in range(1, rows_a):
                sem = fwd_send.at[0, part, (dx - 1) * (rows_a - 1) + dy - 1]
                sends.append(remote(src, 0, part, sem, at(dy, 0)))
                sends[-1].start()
        for dy in range(1, rows_a):
            src = at(dy, 0)
            remote(src, 1, part, own_send.at[0, part, 0], partner).wait_recv()
            for dx in range(1, rows_b):
                sem = fwd_send.at[1, part, (dx - 1) * (rows_a - 1) + dy - 1]
                sends.append(remote(src, 1, part, sem, at(0, dx)))
                sends[-1].start()

    send_own(0)

    loads[2].wait()
    for piece in range(2):
        rows = pl.ds(piece * half, half)
        loads[3 + 2 * piece].wait()
        key_fresh = jnp.dot(hid[rows, :], wk[...], preferred_element_type=jnp.float32)
        fresh[0, rows, :] = key_fresh.astype(jnp.bfloat16)
        key_shift = key_fresh - ck[rows, :].astype(jnp.float32)
        square = key_shift * key_shift
        if piece == 0:
            loads[4].wait()
        value_fresh = jnp.dot(hid[rows, :], wv[...], preferred_element_type=jnp.float32)
        fresh[1, rows, :] = value_fresh.astype(jnp.bfloat16)
        value_shift = value_fresh - cv[rows, :].astype(jnp.float32)
        square = square + value_shift * value_shift
        folded = square[:, 0:HEAD_DIM]
        for h in range(1, local_heads):
            folded = folded + square[:, h * HEAD_DIM:(h + 1) * HEAD_DIM]
        total = jnp.sum(folded.T, axis=0, keepdims=True)
        dev_ref[:, piece * half:(piece + 1) * half] = jnp.broadcast_to(total, (8, half))

    last_row = lax.broadcasted_iota(jnp.int32, (tok - cut, tok), 0) + cut
    hit = last_row == target
    old = jnp.where(hit & (last_row < plain), 1.0, 0.0).astype(jnp.bfloat16)
    new = jnp.where(hit & (last_row >= plain), 1.0, 0.0).astype(jnp.bfloat16)
    for arr, cached in enumerate((ck, cv)):
        tail = jnp.dot(old, cached[...], preferred_element_type=jnp.float32)
        tail = tail + jnp.dot(new, fresh[arr], preferred_element_type=jnp.float32)
        bufs[arr][me, cut:tok, :] = tail.astype(jnp.bfloat16)
    devbuf[zme] = dev_ref[...]
    send_own(1)
    forward(0)
    for d in range(1, kz):
        sends.append(
            pltpu.make_async_remote_copy(
                src_ref=devbuf.at[zme], dst_ref=devbuf.at[zme], send_sem=z_send.at[d - 1],
                recv_sem=z_recv.at[zme], device_id={"kvh": (zme + d) % kz}, device_id_type=MESH,
            )
        )
        sends[-1].start()

    pick = place(plain, pad)
    step = width // 4
    for c in range(4):
        chunk = slice(c * step, (c + 1) * step)
        hq[:, chunk] = jnp.dot(pick, hid[:, chunk], preferred_element_type=jnp.float32).astype(
            jnp.bfloat16
        )
    loads[6].wait()

    def project(h, carry):
        chunk = pl.ds(pl.multiple_of(h * GROUP * HEAD_DIM, HEAD_DIM), GROUP * HEAD_DIM)
        queries = jnp.dot(hq[...], wq[:, chunk], preferred_element_type=jnp.float32).astype(
            jnp.bfloat16
        )
        for g in range(GROUP):
            q_ref[h, g * pad:(g + 1) * pad, :] = queries[:, g * HEAD_DIM:(g + 1) * HEAD_DIM]
        return carry

    lax.fori_loop(0, local_heads, project, 0)

    code = jnp.where(
        lax.broadcasted_iota(jnp.int32, (8, tok), 0) == 0, lane % 256, lane // 256
    ).astype(jnp.float32).astype(jnp.bfloat16)
    found = lax.dot_general(code, place(0, tok), NT, preferred_element_type=jnp.float32)
    key_pos = (found[0:1] + 256.0 * found[1:2]).astype(jnp.int32)
    pad_lane = lax.broadcasted_iota(jnp.int32, (pad, tok), 1)
    row_pos = jnp.sum(
        jnp.where(pick.astype(jnp.float32) > 0, pad_lane.astype(jnp.float32), 0.0),
        axis=1, keepdims=True,
    ).astype(jnp.int32)
    bias_ref[...] = jnp.where(key_pos <= row_pos, 0.0, -1e30)

    chunks = 1
    crows = qrows // chunks

    def attend(src, h, c, keys, own):
        rows = slice(c * crows, (c + 1) * crows)
        head = slice(h * HEAD_DIM, (h + 1) * HEAD_DIM)
        scores = lax.dot_general(
            q_ref[h, rows, :], kbuf[src, keys, head], NT, preferred_element_type=jnp.float32
        )
        if own:
            scores = scores + jnp.concatenate([bias_ref[...]] * (crows // pad), axis=0)
        best = jnp.max(scores, axis=1, keepdims=True)
        if not own:
            before = m_ref[h, rows, :]
            best = jnp.maximum(best, before)
        weights = jnp.exp2((scores - best) * EXP_SCALE)
        row_sum = jnp.sum(weights, axis=1, keepdims=True)
        mixed = jnp.dot(
            weights.astype(jnp.bfloat16), vbuf[src, keys, head], preferred_element_type=jnp.float32
        )
        if not own:
            fade = jnp.exp2((before - best) * EXP_SCALE)
            row_sum = row_sum + l_ref[h, rows, :] * fade
            mixed = mixed + acc_ref[h, rows, :] * fade
        m_ref[h, rows, :] = best
        l_ref[h, rows, :] = row_sum
        acc_ref[h, rows, :] = mixed

    def attend_all(src, first, count, own):
        for h in range(local_heads):
            for c in range(chunks):
                attend(src, h, c, slice(first, first + count), own)

    attend_all(me, 0, tok, True)

    for d in range(1, kz):
        src = (zme + d) % kz
        pltpu.make_async_remote_copy(
            src_ref=devbuf.at[src], dst_ref=devbuf.at[src], send_sem=z_send.at[0],
            recv_sem=z_recv.at[src], device_id={"kvh": src}, device_id_type=MESH,
        ).wait_recv()
    deviation = devbuf[0]
    for z in range(1, kz):
        deviation = deviation + devbuf[z]
    deviation = deviation[0:1]
    position = lane[0:1] + me * tok
    inside = []
    end = jnp.int32(0)
    for d in range(docs):
        begin, end = end, end + lens_ref[d]
        inside.append((position >= begin) & (position < end))
    slot_row = lax.broadcasted_iota(jnp.int32, docbuf.shape[1:], 0)
    shares = jnp.zeros(docbuf.shape[1:], jnp.float32)
    for d in range(docs):
        share = jnp.sum(jnp.where(inside[d], deviation, 0.0), axis=1, keepdims=True)
        shares = jnp.where(slot_row == d, share, shares)
    docbuf[me] = shares
    for d in range(1, n):
        sends.append(
            pltpu.make_async_remote_copy(
                src_ref=docbuf.at[me], dst_ref=docbuf.at[me], send_sem=doc_send.at[d - 1],
                recv_sem=doc_recv.at[me], device_id={"seq": (me + d) % n}, device_id_type=MESH,
            )
        )
        sends[-1].start()

    def other(part, s, carry):
        dc = s % 2
        dx = (s // 2) % rows_b
        dy = s // (2 * rows_b)
        src = at(dy, dx, dc)
        idle = own_send.at[0, part, 0]

        @pl.when((dc == 1) | (dy != 0))
        def _():
            remote(src, 0, part, idle, partner).wait_recv()

        @pl.when((dc == 1) | (dx != 0))
        def _():
            remote(src, 1, part, idle, partner).wait_recv()

        @pl.when(dc == 0)
        def _():
            relay(src, s // 2, part)

        @pl.when(src < me)
        def _():
            attend_all(src, *parts[part], False)

        return carry

    lax.fori_loop(1, n - 2, functools.partial(other, 0), 0)
    forward(1)
    lax.fori_loop(n - 2, n, functools.partial(other, 0), 0)
    lax.fori_loop(1, n, functools.partial(other, 1), 0)

    for h in range(local_heads):
        done = (acc_ref[h] / l_ref[h]).astype(jnp.bfloat16)
        for g in range(GROUP):
            head = h * GROUP + g
            out_ref[:, head * HEAD_DIM:(head + 1) * HEAD_DIM] = done[g * pad:g * pad + sel_rows]

    for d in range(1, n):
        src = (me + d) % n
        pltpu.make_async_remote_copy(
            src_ref=docbuf.at[src], dst_ref=docbuf.at[src], send_sem=doc_send.at[0],
            recv_sem=doc_recv.at[src], device_id={"seq": src}, device_id_type=MESH,
        ).wait_recv()
    totals = docbuf[0]
    for s in range(1, n):
        totals = totals + docbuf[s]
    mean = jnp.zeros((1, tok), jnp.float32)
    for d in range(docs):
        here = totals[d:d + 1, 0:1] / lens_ref[d].astype(jnp.float32)
        mean = jnp.where(inside[d], here, mean)
    score_ref[...] = deviation / (mean + 1.0)

    for send in sends:
        send.wait_send()

    def drain(s, carry):
        for part in (0, 1):
            for arr in (0, 1):
                remote(me, arr, part, relay_send.at[s, arr, part], partner).wait_send()
        return carry

    lax.fori_loop(0, n // 2, drain, 0)


def shards(n, kz, hidden, w_query, w_key, w_value, cached_key, cached_value, doc_lengths, selected):
    tok, width = hidden.shape
    cols = w_key.shape[1]
    qcols = w_query.shape[1]
    sel_rows = selected.shape[0] // n
    docs = doc_lengths.shape[0]
    pad = round_up(sel_rows, 16)
    local_heads = cols // HEAD_DIM
    qrows = GROUP * pad
    rows_a, rows_b = split_chips(n // 2)
    peers = max(1, rows_a + rows_b - 2)
    forwards = max(1, (rows_a - 1) * (rows_b - 1))
    bf, f32 = jnp.bfloat16, jnp.float32
    dma = pltpu.SemaphoreType.DMA
    any_space = pl.BlockSpec(memory_space=pl.ANY)
    vmem = pl.BlockSpec(memory_space=pltpu.VMEM)
    smem = pl.BlockSpec(memory_space=pltpu.SMEM)
    attended, score = pl.pallas_call(
        functools.partial(kernel, n, kz, docs, sel_rows),
        out_shape=(
            jax.ShapeDtypeStruct((sel_rows, qcols), bf),
            jax.ShapeDtypeStruct((1, tok), f32),
        ),
        in_specs=[any_space] * 6 + [smem] * 2,
        out_specs=(vmem, vmem),
        scratch_shapes=[
            pltpu.VMEM((tok, width), bf),
            pltpu.VMEM((width, qcols), bf),
            pltpu.VMEM((width, cols), bf),
            pltpu.VMEM((width, cols), bf),
            pltpu.VMEM((tok, cols), bf),
            pltpu.VMEM((tok, cols), bf),
            pltpu.VMEM((n, tok, cols), bf),
            pltpu.VMEM((n, tok, cols), bf),
            pltpu.VMEM((2, tok, cols), bf),
            pltpu.VMEM((pad, width), bf),
            pltpu.VMEM((local_heads, qrows, HEAD_DIM), bf),
            pltpu.VMEM((local_heads, qrows, 1), f32),
            pltpu.VMEM((local_heads, qrows, 1), f32),
            pltpu.VMEM((local_heads, qrows, HEAD_DIM), f32),
            pltpu.VMEM((8, tok), f32),
            pltpu.VMEM((pad, tok), f32),
            pltpu.VMEM((kz, 8, tok), f32),
            pltpu.VMEM((n, round_up(docs, 8), 128), f32),
            dma((7,)),
            dma((2, 2, peers)),
            dma((2, 2, forwards)),
            dma((n // 2, 2, 2)),
            dma((max(1, kz - 1),)),
            dma((n - 1,)),
            dma((n, 2, 2)),
            dma((kz,)),
            dma((n,)),
        ],
        compiler_params=pltpu.CompilerParams(
            collective_id=0, has_side_effects=True, vmem_limit_bytes=62 * 1024 * 1024
        ),
        name="blend",
    )(hidden, w_query, w_key, w_value, cached_key, cached_value, doc_lengths, selected)
    return attended, score.reshape(tok)


def solution(mesh):
    return jax.shard_map(
        functools.partial(shards, mesh.shape["seq"], mesh.shape["kvh"]),
        mesh=mesh,
        in_specs=(
            P("seq", None),
            P(None, "kvh"),
            P(None, "kvh"),
            P(None, "kvh"),
            P("seq", "kvh"),
            P("seq", "kvh"),
            P(),
            P(),
        ),
        out_specs=(P("seq", "kvh"), P("seq")),
        check_vma=False,
    )
```
